32 devices in a mesh: band: 8 (over z, x), coef: 4 (over y, core).
Axes of the slice: x: 2, y: 2, z: 4, core: 2. Of those that a mesh axis runs over, the one named last changes fastest.
Arguments:
- coeffs: float32 [1024, 262144], P('band', 'coef'), may hold values from -320 to 320
- ref_block: float32 [1024, 262144], P('band', 'coef'), may hold values from -0.01171875 to 0.01171875
- index_map: int32 [262144], P('coef'), may hold values from 0 to 65535, as said below
- band_group: int32 [1024], P('band'), may hold values from 0 to 15
Outputs:
- ortho: float32 [1024, 262144], P('band', 'coef')
- band_residual: float32 [1024], P('band')
- group_residual: float32 [16], replicated
The draws below stay inside these ranges and needn't reach their ends.
Inputs may be any that keep to these rules, and one draw needn't show every extreme that they name: Within each aligned slab of 65536 coefficients, index_map holds every number of 0 to 65535 once.
All inputs are finite; a program needn't handle non-finite values.
Results may differ from the reference program's by a relative error of at most 0.000098.
Values sent between devices are 32-bit elements; how exact they have to be, the bound alone decides.
No kernel may reach another device: no remote copies, remote signals or barrier semaphores. Data moves between devices by JAX's collectives and lax.ppermute only.
A program may use at most 384 MiB of HBM per device.

```python
import math
import jax
import jax.numpy as jnp
from jax import lax

NB = 1024
NG = 262144
NGROUPS = 16
GS = 65536


def shared_basis(key):
    base = jax.random.fold_in(key, 11)
    basis = jnp.clip(jax.random.normal(base, (NB, NG), jnp.float32), -6.0, 6.0)
    return basis


def slab_order(key):
    base = jax.random.fold_in(key, 23)
    slabs = NG // GS
    starts = jnp.arange(slabs)
    keys = jax.vmap(lambda number: jax.random.fold_in(base, number))(starts)
    return jax.vmap(lambda single: jax.random.permutation(single, GS))(keys).astype(jnp.int32)


def draw_coeffs(key, part):
    basis = shared_basis(key)
    mixing = jax.random.uniform(jax.random.fold_in(key, 31), (NB,), jnp.float32, 0.3, 0.6)
    scales = jnp.exp(jax.random.uniform(jax.random.fold_in(key, 37), (NB,), jnp.float32, 0.0, math.log(10.0)))
    mixed = basis + mixing[:, None] * jnp.roll(basis, 1, axis=0)
    return (scales[:, None] * mixed).astype(jnp.float32)


def draw_ref_block(key, part):
    basis = shared_basis(key)
    order = slab_order(key)
    slabs = NG // GS
    shaped = basis.reshape(NB, slabs, GS)
    moved = jnp.take_along_axis(shaped, order[None, :, :], axis=2).reshape(NB, NG)
    return (moved / math.sqrt(NG)).astype(jnp.float32)


def draw_index_map(key, part):
    return slab_order(key).reshape(NG).astype(jnp.int32)


def touch_ends(values, own_key, least, top_value):
    longest = values.shape.index(max(values.shape))
    spots = []
    for shift in (0, 1):
        where = [jax.random.randint(jax.random.fold_in(own_key, axis), (), 0, length) for axis, length in enumerate(values.shape)]
        where[longest] = (where[longest] + shift) % values.shape[longest]
        spots.append(tuple(where))
    return values.at[spots[0]].set(least).at[spots[1]].set(top_value)


def setup_inputs(seed: int = 0) -> dict:
    streams_of = jax.random.split(jax.random.key(seed), 5)
    coeffs = draw_coeffs(jax.random.fold_in(streams_of[4], 71), 0)
    ref_block = draw_ref_block(jax.random.fold_in(streams_of[4], 71), 0)
    index_map = draw_index_map(jax.random.fold_in(streams_of[4], 71), 0)
    band_group = touch_ends(jax.random.randint(streams_of[3], (NB,), 0, NGROUPS), jax.random.fold_in(streams_of[3], 1), 0, NGROUPS - 1).astype(jnp.int32)
    return dict(coeffs=coeffs, ref_block=ref_block, index_map=index_map, band_group=band_group)


def reference(coeffs, ref_block, index_map, band_group):
    margin = jnp.dot(coeffs.astype(jnp.float32), coeffs.T.astype(jnp.float32), precision=lax.Precision.HIGHEST, preferred_element_type=jnp.float32)
    factor = jnp.linalg.cholesky(margin)
    ortho = lax.linalg.triangular_solve(factor, coeffs, left_side=True, lower=True)
    slabs = NG // GS
    shaped = ortho.reshape(NB, slabs, GS)
    order = index_map.reshape(slabs, GS).astype(jnp.int32)
    aligned = jnp.take_along_axis(shaped, order[None, :, :], axis=2).reshape(NB, NG)
    squares = lax.optimization_barrier(jnp.sum((aligned - ref_block) ** 2, axis=1))
    band_residual = jnp.sqrt(squares + 1e-06)
    group_residual = jax.ops.segment_sum(band_residual, band_group, num_segments=NGROUPS) * (NGROUPS / NB)
    return (ortho, band_residual, group_residual.astype(jnp.float32))
```

```python
import functools
import jax
import jax.numpy as jnp
from jax import lax
from jax.experimental import pallas as pl
from jax.experimental.pallas import tpu as pltpu
from jax.sharding import PartitionSpec as P


NGROUPS = 16
UNITS = 16
PIECES = (2, 5, 5, 3, 1)
STAGES = (
    ("across", 1),
    ("within", 0),
    ("across", 2),
    ("added", 0),
    ("across", 3),
    ("within", 1),
    ("within", 2),
    ("across", 4),
    ("within", 3),
    ("within", 4),
)
TILE = 128
ROWS = 256
RANK = 4
STRETCH = 2048
UNROLL = 32
HIGHEST = lax.Precision.HIGHEST


def dot(a, b, dims):
    return lax.dot_general(a, b, (dims, ((), ())), precision=HIGHEST, preferred_element_type=jnp.float32)


def inverse_factor_kernel(packed_ref, out_ref, work, left, right):
    size = out_ref.shape[0]
    start = 0
    for index in range(size // ROWS):
        width = (index + 1) * ROWS
        work[index * ROWS:(index + 1) * ROWS, :width] = packed_ref[:, start:start + width]
        start += width
    rows = lax.broadcasted_iota(jnp.int32, (TILE, TILE), 0)
    lanes = lax.broadcasted_iota(jnp.int32, (TILE, TILE), 1)
    row_lanes = lax.broadcasted_iota(jnp.int32, (1, TILE), 1)
    tall_rows = lax.broadcasted_iota(jnp.int32, (size, TILE), 0)
    wide_lanes = lax.broadcasted_iota(jnp.int32, (TILE, size), 1)

    def block(index, carry):
        base = pl.multiple_of(index * TILE, TILE)
        left[...] = work[pl.ds(base, TILE), pl.ds(base, TILE)]
        right[...] = jnp.where(rows == lanes, 1.0, 0.0).astype(jnp.float32)

        def eliminate(step, inner):
            first = step * RANK
            current = left[...]
            strips = [left[pl.ds(first + t, 1), :] for t in range(RANK)]
            others = [right[pl.ds(first + t, 1), :] for t in range(RANK)]
            cols = [
                jnp.sum(jnp.where(lanes == first + t, current, 0.0), axis=1, keepdims=True)
                for t in range(RANK)
            ]
            core = [
                [
                    jnp.sum(jnp.where(row_lanes == first + u, strips[t], 0.0), axis=1, keepdims=True)
                    for u in range(RANK)
                ]
                for t in range(RANK)
            ]
            updated = right[...]
            for t in range(RANK):
                reciprocal = 1.0 / core[t][t]
                factor = jnp.where(rows > first + t, cols[t] * reciprocal, 0.0)
                for u in range(t + 1, RANK):
                    cols[u] = cols[u] - cols[t] * (reciprocal * core[t][u])
                    ratio = core[u][t] * reciprocal
                    strips[u] = strips[u] - ratio * strips[t]
                    others[u] = others[u] - ratio * others[t]
                    for v in range(t + 1, RANK):
                        core[u][v] = core[u][v] - ratio * core[t][v]
                current = current - factor * strips[t]
                updated = updated - factor * others[t]
            left[...] = current
            right[...] = updated
            return inner

        lax.fori_loop(0, TILE // RANK, eliminate, 0)
        pivots = jnp.sum(jnp.where(rows == lanes, left[...], 0.0), axis=1, keepdims=True)
        scale = lax.rsqrt(pivots)
        scale = scale * (1.5 - 0.5 * pivots * scale * scale)
        corner = right[...] * scale
        panel = dot(work[:, pl.ds(base, TILE)], corner, ((1,), (1,)))
        panel = jnp.where(tall_rows >= base + TILE, panel, 0.0)
        strip = jnp.where(wide_lanes < base, work[pl.ds(base, TILE), :], 0.0)
        strip = dot(corner, strip, ((1,), (0,)))
        work[:, pl.ds(base, TILE)] = jnp.zeros((size, TILE), jnp.float32)
        work[pl.ds(base, TILE), :] = strip
        work[pl.ds(base, TILE), pl.ds(base, TILE)] = corner
        strip = work[pl.ds(base, TILE), :] + panel.T
        work[...] = work[...] - dot(panel, strip, ((1,), (0,)))
        return carry

    lax.fori_loop(0, size // TILE, block, 0)
    shape = (size, size)
    below = lax.broadcasted_iota(jnp.int32, shape, 0) >= lax.broadcasted_iota(jnp.int32, shape, 1)
    out_ref[...] = jnp.where(below, work[...], 0.0)


def inverse_factor(packed, size):
    return pl.pallas_call(
        inverse_factor_kernel,
        out_shape=jax.ShapeDtypeStruct((size, size), jnp.float32),
        in_specs=[pl.BlockSpec(memory_space=pltpu.VMEM)],
        out_specs=pl.BlockSpec(memory_space=pltpu.VMEM),
        scratch_shapes=[
            pltpu.VMEM((size, size), jnp.float32),
            pltpu.VMEM((TILE, TILE), jnp.float32),
            pltpu.VMEM((TILE, TILE), jnp.float32),
        ],
        compiler_params=pltpu.CompilerParams(vmem_limit_bytes=48 * 1024 * 1024),
        name="inverse_factor",
    )(packed)


def rearrange_kernel(index_ref, block_ref, out_ref, table, turned):
    step = pl.program_id(0)
    count = pl.num_programs(0) // 2
    stretch = turned.shape[0]

    @pl.when(step < count)
    def scatter():
        turned[...] = block_ref[...].T

        def group(number, carry):
            base = pl.multiple_of(number * UNROLL, UNROLL)
            for t in range(UNROLL):
                table[pl.ds(index_ref[base + t], 1), :] = turned[pl.ds(base + t, 1), :]
            return carry

        lax.fori_loop(0, stretch // UNROLL, group, 0)

    @pl.when(step >= count)
    def write():
        base = pl.multiple_of((step - count) * stretch, stretch)
        out_ref[...] = table[pl.ds(base, stretch), :].T


def rearrange(index_map, values):
    bands, width = values.shape
    count = width // STRETCH
    return pl.pallas_call(
        rearrange_kernel,
        grid=(2 * count,),
        out_shape=jax.ShapeDtypeStruct(values.shape, values.dtype),
        in_specs=[
            pl.BlockSpec((STRETCH,), lambda i: (jnp.minimum(i, count - 1),), memory_space=pltpu.SMEM),
            pl.BlockSpec((bands, STRETCH), lambda i: (0, jnp.minimum(i, count - 1))),
        ],
        out_specs=pl.BlockSpec((bands, STRETCH), lambda i: (0, jnp.maximum(i - count, 0))),
        scratch_shapes=[
            pltpu.VMEM((width, bands), values.dtype),
            pltpu.VMEM((STRETCH, bands), values.dtype),
        ],
        compiler_params=pltpu.CompilerParams(vmem_limit_bytes=48 * 1024 * 1024),
        name="rearrange",
    )(index_map, values)


def sum_everywhere(value, axes):
    trail = []
    for axis, count in axes:
        place, step = lax.axis_index(axis), 1
        while step < count:
            pairs = [(i, i ^ step) for i in range(count)]
            rows = value.shape[0] // 2
            high = lax.rem(place // step, 2) == 1
            given = lax.dynamic_slice_in_dim(value, jnp.where(high, 0, rows), rows, 0)
            kept = lax.dynamic_slice_in_dim(value, jnp.where(high, rows, 0), rows, 0)
            value = kept + lax.ppermute(given, axis, pairs)
            trail.append((axis, pairs, high))
            step *= 2
    for axis, pairs, high in reversed(trail):
        got = lax.ppermute(value, axis, pairs)
        first, second = jnp.where(high, got, value), jnp.where(high, value, got)
        value = jnp.concatenate([first, second], axis=0)
    return value


def sum_small(value, axes):
    for axis, count in axes:
        step = 1
        while step < count:
            value = value + lax.ppermute(value, axis, [(i, i ^ step) for i in range(count)])
            step *= 2
    return value


def local(axes, coeffs, ref_block, index_map, band_group):
    bands, width = coeffs.shape
    parts = dict(axes)["band"]
    half = parts // 2
    size = bands * parts
    own = width // parts
    unit = own // UNITS
    offsets = [sum(PIECES[:k]) * unit for k in range(len(PIECES))]
    widths = [piece * unit for piece in PIECES]
    extra = widths[0]
    me = lax.axis_index("band")
    place = lax.rem(me, half)
    lower = me >= half

    def shift(value, step):
        return lax.ppermute(value, "band", [(i, i ^ step) for i in range(parts)])

    def take(row, column, rows, columns):
        return lax.dynamic_slice(coeffs, (row, column), (rows, columns))

    def put(buffer, value, row, column):
        return lax.dynamic_update_slice(buffer, value, (row, column))

    moved = rearrange(index_map, ref_block)

    columns, total = [], None
    for k in range(len(PIECES)):
        buffer = jnp.zeros((size, widths[k]), jnp.float32)
        buffer = put(buffer, take(0, me * own + offsets[k], bands, widths[k]), me * bands, 0)
        for step in reversed(range(1, parts)):
            peer = me ^ step
            got = shift(take(0, peer * own + offsets[k], bands, widths[k]), step)
            buffer = put(buffer, got, peer * bands, 0)
        columns.append(buffer)
        blocks = [
            dot(buffer[i:i + ROWS], buffer[:i + ROWS], ((1,), (1,))) for i in range(0, size, ROWS)
        ]
        packed = jnp.concatenate(blocks, axis=1)
        total = packed if total is None else total + packed

    margin = sum_everywhere(total, axes)
    margin, early = lax.optimization_barrier((margin, columns[0][:size // 2]))
    upper = lax.ppermute(early, "band", [(i, i + half) for i in range(half)])

    partner = me ^ half
    side = jnp.zeros((size // 2, extra), jnp.float32)
    side = put(side, take(0, partner * own, bands, extra), place * bands, 0)
    for step in range(1, half):
        peer = me ^ step
        got = shift(take(0, (peer ^ half) * own, bands, extra), step)
        side = put(side, got, lax.rem(peer, half) * bands, 0)
    upper = jnp.where(lower, upper, side)

    inverse_l = inverse_factor(margin, size)
    begin = jnp.where(lower, size // 2, 0)
    mine = lax.dynamic_slice(inverse_l, (begin, 0), (size // 2, size))
    theirs = lax.dynamic_slice(inverse_l, (size // 2 - begin, 0), (size // 2, size))

    ortho = jnp.zeros((bands, width), jnp.float32)
    squares = jnp.zeros((bands,), jnp.float32)
    pieces = []

    def rows_of(value, peer):
        return lax.dynamic_slice(value, (lax.rem(peer, half) * bands, 0), (bands, value.shape[1]))

    sliced = None
    for kind, k in STAGES:
        factor = theirs if kind == "across" else mine
        operand = jnp.concatenate([upper, side], axis=0) if kind == "added" else columns[k]
        if sliced is not None:
            factor, sliced = lax.optimization_barrier((factor, sliced))
            pieces[-1][0] = sliced
        value = dot(factor, operand, ((1,), (0,)))
        steps = range(half, parts) if kind == "across" else range(half)
        sliced = lax.optimization_barrier([rows_of(value, me ^ step) for step in steps])
        flip = half if kind == "added" else 0
        pieces.append([sliced, steps, [(me ^ step ^ flip) * own + offsets[k] for step in steps]])
    for sliced, steps, places in pieces:
        values = [shift(part, step) if step else part for part, step in zip(sliced, steps)]
        values, squares = lax.optimization_barrier((values, squares))
        for value, column in zip(values, places):
            ortho = put(ortho, value, 0, column)
            target = lax.dynamic_slice(moved, (0, column), value.shape)
            squares = squares + jnp.sum((value - target) ** 2, axis=1)

    band_residual = jnp.sqrt(sum_small(squares, axes[:1]) + 1e-06)
    hot = band_group[None, :] == jnp.arange(NGROUPS, dtype=jnp.int32)[:, None]
    terms = jnp.sum(jnp.where(hot, band_residual[None, :], 0.0), axis=1)
    group_residual = sum_small(terms, axes[1:]) * (NGROUPS / size)
    return (ortho, band_residual, group_residual)


def run(axes, *arrays):
    return local(axes, *arrays)


def solution(mesh):
    return jax.shard_map(
        functools.partial(run, tuple((name, mesh.shape[name]) for name in ("coef", "band"))),
        mesh=mesh,
        in_specs=(P("band", "coef"), P("band", "coef"), P("coef"), P("band")),
        out_specs=(P("band", "coef"), P("band"), P()),
        check_vma=False,
    )
```

```python
import functools
import jax
import jax.numpy as jnp
from jax import lax
from jax.experimental import pallas as pl
from jax.experimental.pallas import tpu as pltpu
from jax.sharding import PartitionSpec as P


NGROUPS = 16
UNITS = 16
PIECES = (2, 5, 4, 3, 1, 1)
STAGES = (
    ("across", 5),
    ("across", 1),
    ("within", 0),
    ("across", 2),
    ("added", 0),
    ("within", 1),
    ("across", 3),
    ("within", 2),
    ("within", 3),
    ("within", 5),
    ("across", 4),
    ("within", 4),
)
TILE = 128
ROWS = 256
RANK = 4
STRETCH = 2048
UNROLL = 32
HIGHEST = lax.Precision.HIGHEST


def dot(a, b, dims):
    return lax.dot_general(a, b, (dims, ((), ())), precision=HIGHEST, preferred_element_type=jnp.float32)


def inverse_factor_kernel(packed_ref, out_ref, work, left, right):
    size = out_ref.shape[0]
    start = 0
    for index in range(size // ROWS):
        width = (index + 1) * ROWS
        work[index * ROWS:(index + 1) * ROWS, :width] = packed_ref[:, start:start + width]
        start += width
    rows = lax.broadcasted_iota(jnp.int32, (TILE, TILE), 0)
    lanes = lax.broadcasted_iota(jnp.int32, (TILE, TILE), 1)
    row_lanes = lax.broadcasted_iota(jnp.int32, (1, TILE), 1)
    tall_rows = lax.broadcasted_iota(jnp.int32, (size, TILE), 0)
    wide_lanes = lax.broadcasted_iota(jnp.int32, (TILE, size), 1)

    def block(index, carry):
        base = pl.multiple_of(index * TILE, TILE)
        left[...] = work[pl.ds(base, TILE), pl.ds(base, TILE)]
        right[...] = jnp.where(rows == lanes, 1.0, 0.0).astype(jnp.float32)

        def eliminate(step, inner):
            first = step * RANK
            current = left[...]
            strips = [left[pl.ds(first + t, 1), :] for t in range(RANK)]
            others = [right[pl.ds(first + t, 1), :] for t in range(RANK)]
            cols = [
                jnp.sum(jnp.where(lanes == first + t, current, 0.0), axis=1, keepdims=True)
                for t in range(RANK)
            ]
            core = [
                [
                    jnp.sum(jnp.where(row_lanes == first + u, strips[t], 0.0), axis=1, keepdims=True)
                    for u in range(RANK)
                ]
                for t in range(RANK)
            ]
            updated = right[...]
            for t in range(RANK):
                reciprocal = 1.0 / core[t][t]
                factor = jnp.where(rows > first + t, cols[t] * reciprocal, 0.0)
                for u in range(t + 1, RANK):
                    cols[u] = cols[u] - cols[t] * (reciprocal * core[t][u])
                    ratio = core[u][t] * reciprocal
                    strips[u] = strips[u] - ratio * strips[t]
                    others[u] = others[u] - ratio * others[t]
                    for v in range(t + 1, RANK):
                        core[u][v] = core[u][v] - ratio * core[t][v]
                current = current - factor * strips[t]
                updated = updated - factor * others[t]
            left[...] = current
            right[...] = updated
            return inner

        lax.fori_loop(0, TILE // RANK, eliminate, 0)
        pivots = jnp.sum(jnp.where(rows == lanes, left[...], 0.0), axis=1, keepdims=True)
        scale = lax.rsqrt(pivots)
        scale = scale * (1.5 - 0.5 * pivots * scale * scale)
        corner = right[...] * scale
        panel = dot(work[:, pl.ds(base, TILE)], corner, ((1,), (1,)))
        panel = jnp.where(tall_rows >= base + TILE, panel, 0.0)
        strip = jnp.where(wide_lanes < base, work[pl.ds(base, TILE), :], 0.0)
        strip = dot(corner, strip, ((1,), (0,)))
        work[:, pl.ds(base, TILE)] = jnp.zeros((size, TILE), jnp.float32)
        work[pl.ds(base, TILE), :] = strip
        work[pl.ds(base, TILE), pl.ds(base, TILE)] = corner
        strip = work[pl.ds(base, TILE), :] + panel.T
        work[...] = work[...] - dot(panel, strip, ((1,), (0,)))
        return carry

    lax.fori_loop(0, size // TILE, block, 0)
    shape = (size, size)
    below = lax.broadcasted_iota(jnp.int32, shape, 0) >= lax.broadcasted_iota(jnp.int32, shape, 1)
    out_ref[...] = jnp.where(below, work[...], 0.0)


def inverse_factor(packed, size):
    return pl.pallas_call(
        inverse_factor_kernel,
        out_shape=jax.ShapeDtypeStruct((size, size), jnp.float32),
        in_specs=[pl.BlockSpec(memory_space=pltpu.VMEM)],
        out_specs=pl.BlockSpec(memory_space=pltpu.VMEM),
        scratch_shapes=[
            pltpu.VMEM((size, size), jnp.float32),
            pltpu.VMEM((TILE, TILE), jnp.float32),
            pltpu.VMEM((TILE, TILE), jnp.float32),
        ],
        compiler_params=pltpu.CompilerParams(vmem_limit_bytes=48 * 1024 * 1024),
        name="inverse_factor",
    )(packed)


def rearrange_kernel(index_ref, block_ref, out_ref, table, turned):
    step = pl.program_id(0)
    count = pl.num_programs(0) // 2
    stretch = turned.shape[0]

    @pl.when(step < count)
    def scatter():
        turned[...] = block_ref[...].T

        def group(number, carry):
            base = pl.multiple_of(number * UNROLL, UNROLL)
            for t in range(UNROLL):
                table[pl.ds(index_ref[base + t], 1), :] = turned[pl.ds(base + t, 1), :]
            return carry

        lax.fori_loop(0, stretch // UNROLL, group, 0)

    @pl.when(step >= count)
    def write():
        base = pl.multiple_of((step - count) * stretch, stretch)
        out_ref[...] = table[pl.ds(base, stretch), :].T


def rearrange(index_map, values):
    bands, width = values.shape
    count = width // STRETCH
    return pl.pallas_call(
        rearrange_kernel,
        grid=(2 * count,),
        out_shape=jax.ShapeDtypeStruct(values.shape, values.dtype),
        in_specs=[
            pl.BlockSpec((STRETCH,), lambda i: (jnp.minimum(i, count - 1),), memory_space=pltpu.SMEM),
            pl.BlockSpec((bands, STRETCH), lambda i: (0, jnp.minimum(i, count - 1))),
        ],
        out_specs=pl.BlockSpec((bands, STRETCH), lambda i: (0, jnp.maximum(i - count, 0))),
        scratch_shapes=[
            pltpu.VMEM((width, bands), values.dtype),
            pltpu.VMEM((STRETCH, bands), values.dtype),
        ],
        compiler_params=pltpu.CompilerParams(vmem_limit_bytes=48 * 1024 * 1024),
        name="rearrange",
    )(index_map, values)


def sum_everywhere(value, hops):
    trail = []
    for axis, count, step in hops:
        pairs = [(i, i ^ step) for i in range(count)]
        rows = value.shape[0] // 2
        high = lax.rem(lax.axis_index(axis) // step, 2) == 1
        given = lax.dynamic_slice_in_dim(value, jnp.where(high, 0, rows), rows, 0)
        kept = lax.dynamic_slice_in_dim(value, jnp.where(high, rows, 0), rows, 0)
        value = kept + lax.ppermute(given, axis, pairs)
        trail.append((axis, pairs, high))
    for axis, pairs, high in reversed(trail):
        got = lax.ppermute(value, axis, pairs)
        first, second = jnp.where(high, got, value), jnp.where(high, value, got)
        value = jnp.concatenate([first, second], axis=0)
    return value


def sum_on_two_routes(value, axes):
    hops = []
    for axis, count in axes:
        hops += [(axis, count, 1 << bit) for bit in range(count.bit_length() - 1)]
    other = list(hops)
    for k in range(1, len(hops) - 1, 2):
        other[k], other[k + 1] = hops[k + 1], hops[k]
    middle = value.shape[1] // 2
    return jnp.concatenate(
        [sum_everywhere(value[:, :middle], hops), sum_everywhere(value[:, middle:], other)], axis=1
    )


def sum_small(value, axes):
    for axis, count in axes:
        step = 1
        while step < count:
            value = value + lax.ppermute(value, axis, [(i, i ^ step) for i in range(count)])
            step *= 2
    return value


def local(axes, coeffs, ref_block, index_map, band_group):
    bands, width = coeffs.shape
    parts = dict(axes)["band"]
    half = parts // 2
    size = bands * parts
    own = width // parts
    unit = own // UNITS
    offsets = [sum(PIECES[:k]) * unit for k in range(len(PIECES))]
    widths = [piece * unit for piece in PIECES]
    extra = widths[0]
    me = lax.axis_index("band")
    place = lax.rem(me, half)
    lower = me >= half

    def shift(value, step):
        return lax.ppermute(value, "band", [(i, i ^ step) for i in range(parts)])

    def take(row, column, rows, columns):
        return lax.dynamic_slice(coeffs, (row, column), (rows, columns))

    def put(buffer, value, row, column):
        return lax.dynamic_update_slice(buffer, value, (row, column))

    moved = rearrange(index_map, ref_block)

    columns, total = [], None
    for k in range(len(PIECES)):
        buffer = jnp.zeros((size, widths[k]), jnp.float32)
        buffer = put(buffer, take(0, me * own + offsets[k], bands, widths[k]), me * bands, 0)
        for step in reversed(range(1, parts)):
            peer = me ^ step
            got = shift(take(0, peer * own + offsets[k], bands, widths[k]), step)
            buffer = put(buffer, got, peer * bands, 0)
        columns.append(buffer)
        blocks = [
            dot(buffer[i:i + ROWS], buffer[:i + ROWS], ((1,), (1,))) for i in range(0, size, ROWS)
        ]
        packed = jnp.concatenate(blocks, axis=1)
        total = packed if total is None else total + packed

    margin = sum_on_two_routes(total, axes)
    margin, early = lax.optimization_barrier((margin, columns[0][:size // 2]))
    upper = lax.ppermute(early, "band", [(i, i + half) for i in range(half)])

    partner = me ^ half
    side = jnp.zeros((size // 2, extra), jnp.float32)
    side = put(side, take(0, partner * own, bands, extra), place * bands, 0)
    for step in range(1, half):
        peer = me ^ step
        got = shift(take(0, (peer ^ half) * own, bands, extra), step)
        side = put(side, got, lax.rem(peer, half) * bands, 0)
    upper = jnp.where(lower, upper, side)

    inverse_l = inverse_factor(margin, size)
    begin = jnp.where(lower, size // 2, 0)
    mine = lax.dynamic_slice(inverse_l, (begin, 0), (size // 2, size))
    theirs = lax.dynamic_slice(inverse_l, (size // 2 - begin, 0), (size // 2, size))

    ortho = jnp.zeros((bands, width), jnp.float32)
    squares = jnp.zeros((bands,), jnp.float32)
    pieces = []

    def rows_of(value, peer):
        return lax.dynamic_slice(value, (lax.rem(peer, half) * bands, 0), (bands, value.shape[1]))

    sliced = None
    for kind, k in STAGES:
        factor = theirs if kind == "across" else mine
        operand = jnp.concatenate([upper, side], axis=0) if kind == "added" else columns[k]
        if sliced is not None:
            factor, sliced = lax.optimization_barrier((factor, sliced))
            pieces[-1][0] = sliced
        value = dot(factor, operand, ((1,), (0,)))
        steps = range(half, parts) if kind == "across" else range(half)
        sliced = lax.optimization_barrier([rows_of(value, me ^ step) for step in steps])
        flip = half if kind == "added" else 0
        pieces.append([sliced, steps, [(me ^ step ^ flip) * own + offsets[k] for step in steps]])
    for sliced, steps, places in pieces:
        values = [shift(part, step) if step else part for part, step in zip(sliced, steps)]
        values, squares = lax.optimization_barrier((values, squares))
        for value, column in zip(values, places):
            ortho = put(ortho, value, 0, column)
            target = lax.dynamic_slice(moved, (0, column), value.shape)
            squares = squares + jnp.sum((value - target) ** 2, axis=1)

    band_residual = jnp.sqrt(sum_small(squares, axes[:1]) + 1e-06)
    hot = band_group[None, :] == jnp.arange(NGROUPS, dtype=jnp.int32)[:, None]
    terms = jnp.sum(jnp.where(hot, band_residual[None, :], 0.0), axis=1)
    group_residual = sum_small(terms, axes[1:]) * (NGROUPS / size)
    return (ortho, band_residual, group_residual)


def run(axes, *arrays):
    return local(axes, *arrays)


def solution(mesh):
    return jax.shard_map(
        functools.partial(run, tuple((name, mesh.shape[name]) for name in ("coef", "band"))),
        mesh=mesh,
        in_specs=(P("band", "coef"), P("band", "coef"), P("coef"), P("band")),
        out_specs=(P("band", "coef"), P("band"), P()),
        check_vma=False,
    )
```
